64 devices in a mesh: dp: 8 (over x, y, core), sp: 8 (over z).
Axes of the slice: x: 2, y: 2, z: 8, core: 2. Of those that a mesh axis runs over, the one named last changes fastest.
The devices are a block of a 4x4x8 slice.
Arguments:
- x: bfloat16 [32768, 5376], P(('dp', 'sp')), parts along dimension 0
- gain: bfloat16 [5376], replicated
- wq: bfloat16 [5376, 4096], replicated
- wk: bfloat16 [5376, 2048], replicated
- wv: bfloat16 [5376, 2048], replicated
- wo: bfloat16 [4096, 5376], replicated
Outputs:
- output: bfloat16 [32768, 5376], P(('dp', 'sp')), parts along dimension 0
There are 8 independent parts. The reference program is written for one: setup_inputs(seed, part) draws one part's arguments, and reference() takes and returns one part's arrays. A program takes and returns all parts, laid end to end along the dimension named above; an argument that names none is the same for every part.
All inputs are finite; a program needn't handle non-finite values.
Results may differ from the reference program's by a relative error of at most 0.012.
Values are sent between devices in bfloat16 or wider.
A program may use at most 768 MiB of HBM per device.

```python
import jax
import jax.numpy as jnp
from jax import lax

ROWS = 4096
D = 5376
HEADS = 32
KV_HEADS = 16
HEAD = 128
THETA = 10000


def setup_inputs(seed: int = 0, part: int = 0) -> dict:
    kx, kn, kq, kk, kv, ko = jax.random.split(jax.random.key(seed), 6)

    def weights(key, rows, columns):
        return jax.random.normal(key, (rows, columns), jnp.float32) * rows**-0.5

    drawn = {
        "x": jax.random.normal(jax.random.fold_in(kx, part), (ROWS, D), jnp.float32),
        "gain": 1 + 0.1 * jax.random.normal(kn, (D,), jnp.float32),
        "wq": 2 * weights(kq, D, HEADS * HEAD),
        "wk": 2 * weights(kk, D, KV_HEADS * HEAD),
        "wv": 4 * weights(kv, D, KV_HEADS * HEAD),
        "wo": weights(ko, HEADS * HEAD, D),
    }
    return {k: v.astype(jnp.bfloat16) for k, v in drawn.items()}


def normed(x, gain):
    wide = x.astype(jnp.float32)
    scale = lax.rsqrt(jnp.mean(wide * wide, -1, keepdims=True) + 1e-6)
    return (wide * scale * gain.astype(jnp.float32)).astype(jnp.bfloat16)


def turned(t, place, theta):
    half = t.shape[-1] // 2
    angle = place.astype(jnp.float32)[:, None] * theta ** (-jnp.arange(half, dtype=jnp.float32) / half)
    cos, sin = jnp.cos(angle)[:, None], jnp.sin(angle)[:, None]
    a, b = t[..., :half].astype(jnp.float32), t[..., half:].astype(jnp.float32)
    return jnp.concatenate([a * cos - b * sin, b * cos + a * sin], -1).astype(jnp.bfloat16)


def matmul(a, w):
    return jnp.dot(a, w, preferred_element_type=jnp.float32).astype(jnp.bfloat16)


def einsum(form, a, b):
    return jnp.einsum(form, a.astype(jnp.float32), b.astype(jnp.float32))


def attention(q, k, v):
    scores = einsum("tgsd,ugd->gstu", q, k) * q.shape[-1] ** -0.5
    token = jnp.arange(q.shape[0])
    scores = jnp.where(token[:, None] >= token, scores, -jnp.inf)
    weights = jax.nn.softmax(scores, -1).astype(jnp.bfloat16)
    return einsum("gstu,ugd->tgsd", weights, v).astype(jnp.bfloat16)


def reference(x, gain, wq, wk, wv, wo):
    a, place = normed(x, gain), jnp.arange(ROWS)
    q = turned(matmul(a, wq).reshape(ROWS, HEADS, HEAD), place, THETA).reshape(ROWS, KV_HEADS, -1, HEAD)
    k = turned(matmul(a, wk).reshape(ROWS, KV_HEADS, HEAD), place, THETA)
    v = matmul(a, wv).reshape(ROWS, KV_HEADS, HEAD)
    seen = attention(q, k, v).reshape(ROWS, HEADS * HEAD)
    return (x.astype(jnp.float32) + jnp.dot(seen, wo, preferred_element_type=jnp.float32)).astype(jnp.bfloat16)
```

```python
import functools

import jax
import jax.numpy as jnp
from jax import lax
from jax.experimental import pallas as pl
from jax.experimental.pallas import tpu as pltpu
from jax.sharding import PartitionSpec as P

HEAD = 128
THETA = 10000
NEG = -1e30
HIDDEN = 2 * NEG
LOG2E = 1.4426950408889634
RING = 8
PLANS = [
    0o0123456720377713,
    0o0123456623463255,
    0o0123444473233632,
    0o0133333234220303,
    0o0023456754255746,
    0o0123455554663353,
    0o0122221124104063,
    0o0121221172232357,
    0o0123333233632115,
    0o0103456623364231,
    0o1121377064300371,
    0o0120456712154333,
    0o0123456606532600,
    0o0114556732453636,
    0o0123456713043316,
    0o1011166743001774,
]
START, PROJECT, BLOCK, PIECE, WIRE, FLIGHT = 8.0, 4.0, 0.95, 2.0, 5.6255, 2.0


def _way(a, b):
    d = (b - a) % RING
    return [(0, (a + k) % RING) for k in range(d)] if 2 * d < RING else [(1, (a - k) % RING) for k in range(RING - d)]


def _schedule():
    heads = len(PLANS)
    digits = [[(word >> 3 * (2 * RING - 1 - n)) & 7 for n in range(2 * RING)] for word in PLANS]
    place = [d[:RING] for d in digits]
    own = [[[] for _ in PLANS] for _ in range(RING)]
    relay, todo, need = {}, [[] for _ in range(RING)], {}
    for h, d in enumerate(digits):
        for j in range(RING):
            users = {place[h][i] for i in range(j, RING)}
            for arm in range(2):
                hops = [o for o in range(1, RING) if (o <= d[RING + j] if arm == 0 else RING - o > d[RING + j])]
                chain = [n for n in ((j + o) % RING if arm == 0 else (j - o) % RING for o in hops) if n in users]
                for k, (a, b) in enumerate(zip([j] + chain, chain)):
                    move = ("kv", h, j, a, b, arm)
                    if a == j:
                        own[j][h].append((k - len(chain) - 0.01 * len(_way(a, b)), move))
                    else:
                        relay[h, j, a] = move
            if place[h][j] != j:
                own[j][h].append((-1.5 - 0.01 * len(_way(j, place[h][j])), ("q", h, j, j, place[h][j], 0)))
            m = place[h][j]
            todo[m].append((h, j))
            need[h, j] = {("kv", h, n) for n in range(j + 1) if n != m} | ({("q", h, j)} if j != m else set())
    count = [len(t) for t in todo]
    ops, items, ends = [[] for _ in range(RING)], [[] for _ in range(RING)], [[0] for _ in range(RING)]
    heard = [set() for _ in range(RING)]
    queue = {(m, way): [] for m in range(RING) for way in range(2)}
    live, late, flying = {}, [[] for _ in range(RING)], []
    step, at, idle, busy = [1] * RING, [START + 1.5 * PROJECT] * RING, [False] * RING, [None] * RING
    now = 0.0

    def push(move):
        kind, h, j, a, b, arm = move
        queue[a, _way(a, b)[0][0]].append(move)
        if kind != "o":
            waits = kind == "kv" and a != j
            if waits:
                heard[a].add((h, j))
            ops[a].append(b | j << 3 | h << 6 | waits << 10 | arm << 11 | (kind == "q") << 12)

    def begin(m):
        for h, i in todo[m]:
            if not need[h, i]:
                todo[m].remove((h, i))
                mask = sum(1 << n for n in range(i + 1) if n != m and (h, n) not in heard[m])
                heard[m].update((h, n) for n in range(i + 1))
                items[m].append(i | h << 3 | (i != m) << 7 | mask << 8)
                ends[m].append(len(ops[m]))
                busy[m], idle[m], at[m] = (h, i), False, now + PIECE + BLOCK * (i + 1)
                return
        idle[m], at[m] = True, float("inf")

    while True:
        for key, waiting in queue.items():
            if waiting and key not in live:
                live[key] = [waiting.pop(0), 1.0]
        room, users = {}, {}
        for key, (move, _) in live.items():
            for link in _way(move[3], move[4]):
                room[link] = 1 / WIRE
                users.setdefault(link, set()).add(key)
        rate = {}
        while len(rate) < len(live):
            link = min((n for n in users if users[n]), key=lambda n: room[n] / len(users[n]))
            share = room[link] / len(users[link])
            for key in sorted(users[link]):
                rate[key] = share
                for n in _way(live[key][0][3], live[key][0][4]):
                    room[n] -= share
                    users[n].discard(key)
        then = min([now + left / rate[key] for key, (_, left) in live.items()] + at + [t for t, _ in flying[:1]])
        if then == float("inf"):
            break
        for key in list(live):
            live[key][1] -= rate[key] * (then - now)
            if live[key][1] < 1e-8:
                flying.append((then + FLIGHT, live.pop(key)[0]))
        now = then
        while flying and flying[0][0] <= now + 1e-9:
            kind, h, j, _, m, _ = flying.pop(0)[1]
            if kind == "o":
                continue
            if kind == "kv" and (h, j, m) in relay:
                (push if idle[m] else late[m].append)(relay[h, j, m])
            for i in range(RING):
                if place[h][i] == m:
                    need[h, i].discard((kind, h, j))
            if idle[m]:
                begin(m)
        for m in range(RING):
            while at[m] <= now + 1e-9:
                s = step[m]
                step[m] += 1
                if s <= heads:
                    for _, move in sorted(own[m][s - 1]):
                        push(move)
                elif busy[m] and busy[m][1] != m:
                    push(("o", *busy[m], m, busy[m][1], 0))
                for move in late[m]:
                    push(move)
                late[m] = []
                if s < heads:
                    ends[m].append(len(ops[m]))
                    at[m] = START + (s + 1.5) * PROJECT if s + 1 < heads else START + heads * PROJECT + 0.5
                else:
                    begin(m)
    last = max(count)
    for m in range(RING):
        items[m] += [-1] * (last - len(items[m]))
        ends[m] += [len(ops[m])] * (heads + last + 1 - len(ends[m]))
    longest = max(len(o) for o in ops)
    ops = [o + [0] * (longest - len(o)) for o in ops]
    away = [sum(1 << h for h in range(heads) if place[h][m] != m) for m in range(RING)]
    return *([list(row) for row in zip(*table)] for table in (ops, items, ends)), away, now


OPS, ITEMS, ENDS, AWAY, _ = _schedule()


def _dot(a, b, ca, cb):
    return lax.dot_general(a, b, (((ca,), (cb,)), ((), ())), preferred_element_type=jnp.float32)


def _pick(me, values):
    got = jnp.int32(values[0])
    for d in range(1, len(values)):
        got = jnp.where(me == d, jnp.int32(values[d]), got)
    return got


def _kernel(heads, g, x_ref, gain_ref, cos_ref, sin_ref, wq, wk, wv, o_full, kv_buf, q_buf, a_s, w_s, st_q, st_kv, kvb, q_v, top_s, mix_s, o_st,
            ops_s, items_s, ends_s, kv_r, q_r, o_r, kv_sd, q_sd, o_sd, w_sem, st_sem, ld_sem):
    me = lax.axis_index("sp")
    t, depth = x_ref.shape
    wide = g * HEAD
    low = x_ref.dtype
    other = lax.rem(me + 1, RING)

    barrier = pltpu.get_barrier_semaphore()
    for k in range(1, RING):
        pl.semaphore_signal(barrier, inc=1, device_id={"sp": lax.rem(me + k, RING)}, device_id_type=pl.DeviceIdType.MESH)

    def weights(h, slot):
        q_cols = pl.ds(pl.multiple_of(h * wide, wide), wide)
        cols = pl.ds(pl.multiple_of(h * HEAD, HEAD), HEAD)
        return [pltpu.make_async_copy(wq.at[:, q_cols], w_s.at[slot, :, pl.ds(0, wide)], w_sem.at[slot, 0]),
                pltpu.make_async_copy(wk.at[:, cols], w_s.at[slot, :, pl.ds(wide, HEAD)], w_sem.at[slot, 1]),
                pltpu.make_async_copy(wv.at[:, cols], w_s.at[slot, :, pl.ds(wide + HEAD, HEAD)], w_sem.at[slot, 2])]

    for c in weights(0, 0):
        c.start()

    for p in range(len(OPS)):
        ops_s[p] = _pick(me, OPS[p])
    for p in range(len(ITEMS)):
        items_s[p] = _pick(me, ITEMS[p])
    for p in range(len(ENDS)):
        ends_s[p] = _pick(me, ENDS[p])

    rows = 16
    gain = gain_ref[...].astype(jnp.float32)

    def norm(r, _):
        at = pl.ds(pl.multiple_of(r * rows, rows), rows)
        v = x_ref[at, :].astype(jnp.float32)
        scale = lax.rsqrt(jnp.mean(v * v, -1, keepdims=True) + 1e-6)
        a_s[at, :] = (v * scale * gain).astype(low)
        return _

    lax.fori_loop(0, t // rows, norm, 0)
    pl.semaphore_wait(barrier, RING - 1)

    def kv_copy(h, j, dest, arm):
        at = h * RING + j
        return pltpu.make_async_remote_copy(src_ref=kv_buf.at[h, j], dst_ref=kv_buf.at[h, j], send_sem=kv_sd.at[at * 2 + arm], recv_sem=kv_r.at[at],
                                            device_id={"sp": dest}, device_id_type=pl.DeviceIdType.MESH)

    def q_copy(h, i, dest):
        return pltpu.make_async_remote_copy(src_ref=q_buf.at[h, i], dst_ref=q_buf.at[h, i], send_sem=q_sd.at[h], recv_sem=q_r.at[h * RING + i],
                                            device_id={"sp": dest}, device_id_type=pl.DeviceIdType.MESH)

    def o_copy(h, slot, dest):
        cols = pl.ds(pl.multiple_of(h * wide, wide), wide)
        return pltpu.make_async_remote_copy(src_ref=o_st.at[slot], dst_ref=o_full.at[:, cols], send_sem=o_sd.at[slot], recv_sem=o_r.at[h],
                                            device_id={"sp": dest}, device_id_type=pl.DeviceIdType.MESH)

    def o_local(h, slot):
        cols = pl.ds(pl.multiple_of(h * wide, wide), wide)
        return pltpu.make_async_copy(o_st.at[slot], o_full.at[:, cols], o_sd.at[slot])

    def fields(word):
        return word & 7, (word >> 3) & 7, (word >> 6) & 15, (word >> 10) & 1, (word >> 11) & 1, (word >> 12) & 1

    def send(p, _):
        dest, j, h, waits, arm, queries = fields(ops_s[p])

        @pl.when(queries == 1)
        def _():
            q_copy(h, j, dest).start()

        @pl.when(queries == 0)
        def _():
            @pl.when(waits == 1)
            def _():
                kv_copy(h, j, other, 0).wait_recv()

            kv_copy(h, j, dest, arm).start()

        return 0

    def sends(s):
        lax.fori_loop(0 if isinstance(s, int) and s == 0 else ends_s[s - 1], ends_s[s], send, 0)

    def staged(h, slot):
        return [pltpu.make_async_copy(st_q.at[slot], q_buf.at[h, me], st_sem.at[slot, 0]),
                pltpu.make_async_copy(st_kv.at[slot], kv_buf.at[h, me], st_sem.at[slot, 1])]

    half = t // 2

    def project(h, r, slot):
        at = pl.ds(r * half, half)
        got = _dot(a_s[at, :], w_s[slot], 1, 0).astype(low)
        cos, sin = cos_ref[at, :], sin_ref[at, :]

        def turned(v):
            v = v.astype(jnp.float32)
            return (v * cos + pltpu.roll(v, HEAD // 2, 1) * sin).astype(low)

        for n in range(g):
            st_q[slot, pl.ds(n * t + r * half, half), :] = turned(got[:, n * HEAD : (n + 1) * HEAD])
        st_kv[slot, at, :] = turned(got[:, wide : wide + HEAD])
        for b in range(half // HEAD):
            st_kv[slot, pl.ds(t + r * half + b * HEAD, HEAD), :] = got[b * HEAD : (b + 1) * HEAD, wide + HEAD :].T

    def head(h, _):
        slot = lax.rem(h, 2)
        for c in weights(h, slot):
            c.wait()

        @pl.when(h + 1 < heads)
        def _():
            for c in weights(h + 1, 1 - slot):
                c.start()

        project(h, 0, slot)

        @pl.when(h >= 1)
        def _():
            for c in staged(h - 1, 1 - slot):
                c.wait()
            sends(h)

        project(h, 1, slot)
        for c in staged(h, slot):
            c.start()
        return 0

    lax.fori_loop(0, heads, head, 0)
    for c in staged(heads - 1, (heads - 1) % 2):
        c.wait()

    e = HEAD**-0.5 * LOG2E
    ones = jnp.ones((8, t), low)

    def block(j, masked):
        scores = [_dot(kvb[j, :t, :], q_v[n * t : (n + 1) * t, :], 1, 1) for n in range(g)]
        values = jnp.concatenate([jnp.concatenate([kvb[j, t + b * HEAD : t + (b + 1) * HEAD, :] for b in range(t // HEAD)], axis=1), ones], axis=0)
        kept = []
        for n, s in enumerate(scores):
            at = slice(n * t, (n + 1) * t)
            if masked:
                s = jnp.where(lax.broadcasted_iota(jnp.int32, s.shape, 0) <= lax.broadcasted_iota(jnp.int32, s.shape, 1), s, HIDDEN)
            old = top_s[:, at]
            top = jnp.maximum(old, s.max(axis=0, keepdims=True))
            top_s[:, at] = top
            kept.append((jnp.exp2((s - top) * e).astype(low), jnp.exp2((old - top) * e)))
        for n, (p, keep) in enumerate(kept):
            at = slice(n * t, (n + 1) * t)
            mix_s[:, at] = mix_s[:, at] * keep + _dot(values, p, 1, 0)

    def item(k, _):
        word = items_s[k]
        sends(heads + k)

        @pl.when(word >= 0)
        def _():
            i, h, q_wait, mask = word & 7, (word >> 3) & 15, (word >> 7) & 1, (word >> 8) & 255
            slot = lax.rem(k, 2)
            cp_q = pltpu.make_async_copy(q_buf.at[h, i], q_v, ld_sem.at[RING])

            def cp_kv(j):
                return pltpu.make_async_copy(kv_buf.at[h, j], kvb.at[j], ld_sem.at[j])

            @pl.when(q_wait == 1)
            def _():
                q_copy(h, i, other).wait_recv()

            cp_q.start()

            def arrive(j, _):
                @pl.when(((mask >> j) & 1) == 1)
                def _():
                    kv_copy(h, j, other, 0).wait_recv()

                cp_kv(j).start()
                return 0

            lax.fori_loop(0, i + 1, arrive, 0)
            top_s[...] = jnp.full(top_s.shape, NEG, jnp.float32)
            mix_s[...] = jnp.zeros(mix_s.shape, jnp.float32)
            cp_q.wait()

            def step(j, _):
                cp_kv(j).wait()
                block(j, False)
                return 0

            lax.fori_loop(0, i, step, 0)
            cp_kv(i).wait()
            block(i, True)

            @pl.when(k >= 2)
            def _():
                o_local(h, slot).wait()

            for n in range(g):
                at = slice(n * t, (n + 1) * t)
                o_st[slot, :, n * HEAD : (n + 1) * HEAD] = (mix_s[:HEAD, at] * (1 / mix_s[HEAD : HEAD + 1, at])).T.astype(low)

            @pl.when(i == me)
            def _():
                o_local(h, slot).start()

            @pl.when(i != me)
            def _():
                o_copy(h, slot, i).start()

        return 0

    lax.fori_loop(0, len(ITEMS), item, 0)
    sends(len(ENDS) - 1)

    for slot in range(2):
        o_local(0, slot).wait()

    def sent(p, _):
        dest, j, h, waits, arm, queries = fields(ops_s[p])

        @pl.when(queries == 1)
        def _():
            q_copy(h, j, dest).wait_send()

        @pl.when(queries == 0)
        def _():
            kv_copy(h, j, dest, arm).wait_send()

        return 0

    lax.fori_loop(0, ends_s[len(ENDS) - 1], sent, 0)

    def back(h, _):
        @pl.when(((_pick(me, AWAY) >> h) & 1) == 1)
        def _():
            o_copy(h, 0, other).wait_recv()

        return 0

    lax.fori_loop(0, heads, back, 0)


def attended(x, gain, wq, wk, wv, cos, sin):
    t, depth = x.shape
    heads, g = wk.shape[1] // HEAD, wq.shape[1] // wk.shape[1]
    low = x.dtype
    anywhere, vmem = pl.BlockSpec(memory_space=pl.ANY), pl.BlockSpec(memory_space=pltpu.VMEM)
    dma = pltpu.SemaphoreType.DMA
    out = pl.pallas_call(
        functools.partial(_kernel, heads, g),
        out_shape=[jax.ShapeDtypeStruct((t, wq.shape[1]), low), jax.ShapeDtypeStruct((heads, RING, 2 * t, HEAD), low),
                   jax.ShapeDtypeStruct((heads, RING, g * t, HEAD), low)],
        in_specs=[vmem] * 4 + [anywhere] * 3,
        out_specs=[anywhere] * 3,
        scratch_shapes=[
            pltpu.VMEM((t, depth), low),
            pltpu.VMEM((2, depth, (g + 2) * HEAD), low),
            pltpu.VMEM((2, g * t, HEAD), low),
            pltpu.VMEM((2, 2 * t, HEAD), low),
            pltpu.VMEM((RING, 2 * t, HEAD), low),
            pltpu.VMEM((g * t, HEAD), low),
            pltpu.VMEM((1, g * t), jnp.float32),
            pltpu.VMEM((HEAD + 8, g * t), jnp.float32),
            pltpu.VMEM((2, t, g * HEAD), low),
            pltpu.SMEM((len(OPS),), jnp.int32),
            pltpu.SMEM((len(ITEMS),), jnp.int32),
            pltpu.SMEM((len(ENDS),), jnp.int32),
            dma((heads * RING,)), dma((heads * RING,)), dma((heads,)), dma((heads * RING * 2,)), dma((heads,)), dma((2,)),
            dma((2, 3)), dma((2, 2)), dma((RING + 1,)),
        ],
        compiler_params=pltpu.CompilerParams(collective_id=0, has_side_effects=True, vmem_limit_bytes=60 * 2**20),
    )(x, gain[None], cos, sin, wq, wk, wv)
    return out[0]


def solution(mesh):
    def step(x, gain, wq, wk, wv, wo):
        own = x.shape[0]
        place = lax.axis_index("sp") * own + jnp.arange(own)
        half = HEAD // 2
        angle = place.astype(jnp.float32)[:, None] * THETA ** (-jnp.arange(half, dtype=jnp.float32) / half)
        cos, sin = jnp.cos(angle), jnp.sin(angle)
        seen = attended(x, gain, wq, wk, wv, jnp.concatenate([cos, cos], 1), jnp.concatenate([-sin, sin], 1))
        y = jnp.dot(seen, wo, preferred_element_type=jnp.float32)
        return (x.astype(jnp.float32) + y).astype(jnp.bfloat16)

    tokens, whole = P(("dp", "sp"), None), P(None, None)
    return jax.shard_map(
        step,
        mesh=mesh,
        in_specs=(tokens, P(None), whole, whole, whole, whole),
        out_specs=tokens,
        check_vma=False,
    )
```

```python
import functools

import jax
import jax.numpy as jnp
from jax import lax
from jax.experimental import pallas as pl
from jax.experimental.pallas import tpu as pltpu
from jax.sharding import PartitionSpec as P

HEAD = 128
THETA = 10000
NEG = -1e30
HIDDEN = 2 * NEG
LOG2E = 1.4426950408889634
RING = 8
PLANS = [
    0o0124446621746265,
    0o0114455516332722,
    0o0023330072512457,
    0o0122466632436731,
    0o0114455524472702,
    0o0023330073513376,
    0o0023333276724103,
    0o0122277734200326,
    0o0122666721047474,
    0o0114455536452514,
    0o0133555516466024,
    0o0122666731345773,
    0o0122277764321530,
    0o0122200065341752,
    0o0133331142102343,
    0o0113331154141377,
]
START, PROJECT, BLOCK, PIECE, WIRE, FLIGHT = 8.0, 4.0, 0.95, 2.0, 5.6255, 2.0

MARGIN = 20.0


def _way(a, b):
    d = (b - a) % RING
    return [(0, (a + k) % RING) for k in range(d)] if 2 * d < RING else [(1, (a - k) % RING) for k in range(RING - d)]


def _schedule():
    heads = len(PLANS)
    digits = [[(word >> 3 * (2 * RING - 1 - n)) & 7 for n in range(2 * RING)] for word in PLANS]
    place = [d[:RING] for d in digits]
    own = [[[] for _ in PLANS] for _ in range(RING)]
    relay, todo, need = {}, [[] for _ in range(RING)], {}
    for h, d in enumerate(digits):
        for j in range(RING):
            users = {place[h][i] for i in range(j, RING)}
            for arm in range(2):
                hops = [o for o in range(1, RING) if (o <= d[RING + j] if arm == 0 else RING - o > d[RING + j])]
                chain = [n for n in ((j + o) % RING if arm == 0 else (j - o) % RING for o in hops) if n in users]
                for k, (a, b) in enumerate(zip([j] + chain, chain)):
                    move = ("kv", h, j, a, b, arm)
                    if a == j:
                        own[j][h].append((k - len(chain) - 0.01 * len(_way(a, b)), move))
                    else:
                        relay[h, j, a] = move
            if place[h][j] != j:
                own[j][h].append((-1.5 - 0.01 * len(_way(j, place[h][j])), ("q", h, j, j, place[h][j], 0)))
            m = place[h][j]
            todo[m].append((h, j))
            need[h, j] = {("kv", h, n) for n in range(j + 1) if n != m} | ({("q", h, j)} if j != m else set())
    count = [len(t) for t in todo]
    ops, items, ends = [[] for _ in range(RING)], [[] for _ in range(RING)], [[0] for _ in range(RING)]
    heard = [set() for _ in range(RING)]
    queue = {(m, way): [] for m in range(RING) for way in range(2)}
    live, late, flying = {}, [[] for _ in range(RING)], []
    step, at, idle, busy = [1] * RING, [START + 1.5 * PROJECT] * RING, [False] * RING, [None] * RING
    now, here, begun = 0.0, [0.0] * RING, [[] for _ in range(RING)]

    def push(move):
        kind, h, j, a, b, arm = move
        queue[a, _way(a, b)[0][0]].append(move)
        if kind != "o":
            waits = kind == "kv" and a != j
            if waits:
                heard[a].add((h, j))
            ops[a].append(b | j << 3 | h << 6 | waits << 10 | arm << 11 | (kind == "q") << 12)

    def begin(m):
        for h, i in todo[m]:
            if not need[h, i]:
                todo[m].remove((h, i))
                mask = sum(1 << n for n in range(i + 1) if n != m and (h, n) not in heard[m])
                heard[m].update((h, n) for n in range(i + 1))
                items[m].append(i | h << 3 | (i != m) << 7 | mask << 8)
                ends[m].append(len(ops[m]))
                begun[m].append(now)
                busy[m], idle[m], at[m] = (h, i), False, now + PIECE + BLOCK * (i + 1)
                return
        idle[m], at[m] = True, float("inf")

    while True:
        for key, waiting in queue.items():
            if waiting and key not in live:
                live[key] = [waiting.pop(0), 1.0]
        room, users = {}, {}
        for key, (move, _) in live.items():
            for link in _way(move[3], move[4]):
                room[link] = 1 / WIRE
                users.setdefault(link, set()).add(key)
        rate = {}
        while len(rate) < len(live):
            link = min((n for n in users if users[n]), key=lambda n: room[n] / len(users[n]))
            share = room[link] / len(users[link])
            for key in sorted(users[link]):
                rate[key] = share
                for n in _way(live[key][0][3], live[key][0][4]):
                    room[n] -= share
                    users[n].discard(key)
        then = min([now + left / rate[key] for key, (_, left) in live.items()] + at + [t for t, _ in flying[:1]])
        if then == float("inf"):
            break
        for key in list(live):
            live[key][1] -= rate[key] * (then - now)
            if live[key][1] < 1e-8:
                flying.append((then + FLIGHT, live.pop(key)[0]))
        now = then
        while flying and flying[0][0] <= now + 1e-9:
            kind, h, j, _, m, _ = flying.pop(0)[1]
            if kind == "o":
                if h < heads // 2:
                    here[m] = now
                continue
            if kind == "kv" and (h, j, m) in relay:
                (push if idle[m] else late[m].append)(relay[h, j, m])
            for i in range(RING):
                if place[h][i] == m:
                    need[h, i].discard((kind, h, j))
            if idle[m]:
                begin(m)
        for m in range(RING):
            while at[m] <= now + 1e-9:
                s = step[m]
                step[m] += 1
                if s <= heads:
                    for _, move in sorted(own[m][s - 1]):
                        push(move)
                elif busy[m]:
                    h, i = busy[m]
                    if i != m:
                        push(("o", h, i, m, i, 0))
                    elif h < heads // 2:
                        here[m] = now
                for move in late[m]:
                    push(move)
                late[m] = []
                if s < heads:
                    ends[m].append(len(ops[m]))
                    at[m] = START + (s + 1.5) * PROJECT if s + 1 < heads else START + heads * PROJECT + 0.5
                else:
                    begin(m)
    last = max(count)
    for m in range(RING):
        items[m] += [-1] * (last - len(items[m]))
        ends[m] += [len(ops[m])] * (heads + last + 1 - len(ends[m]))
    longest = max(len(o) for o in ops)
    ops = [o + [0] * (longest - len(o)) for o in ops]
    away = [sum(1 << h for h in range(heads) if place[h][m] != m) for m in range(RING)]
    early = [sum(t < here[m] + MARGIN for t in begun[m]) for m in range(RING)]
    return *([list(row) for row in zip(*table)] for table in (ops, items, ends)), away, early, now


OPS, ITEMS, ENDS, AWAY, EARLY, _ = _schedule()


def _dot(a, b, ca, cb):
    return lax.dot_general(a, b, (((ca,), (cb,)), ((), ())), preferred_element_type=jnp.float32)


def _pick(me, values):
    got = jnp.int32(values[0])
    for d in range(1, len(values)):
        got = jnp.where(me == d, jnp.int32(values[d]), got)
    return got


def _kernel(heads, g, x_ref, gain_ref, cos_ref, sin_ref, wq, wk, wv, wo, y_ref, o_full, kv_buf, q_buf, a_s, w_s, st_q, st_kv, kvb, q_v, top_s, mix_s, o_st,
            ops_s, items_s, ends_s, kv_r, q_r, o_r, kv_sd, q_sd, o_sd, w_sem, st_sem, ld_sem, y_s, wo_s, o_v, y_st, wo_sem, ov_sem, y_sem):
    me = lax.axis_index("sp")
    t, depth = x_ref.shape
    wide = g * HEAD
    low = x_ref.dtype
    other = lax.rem(me + 1, RING)

    barrier = pltpu.get_barrier_semaphore()
    for k in range(1, RING):
        pl.semaphore_signal(barrier, inc=1, device_id={"sp": lax.rem(me + k, RING)}, device_id_type=pl.DeviceIdType.MESH)

    def weights(h, slot):
        q_cols = pl.ds(pl.multiple_of(h * wide, wide), wide)
        cols = pl.ds(pl.multiple_of(h * HEAD, HEAD), HEAD)
        return [pltpu.make_async_copy(wq.at[:, q_cols], w_s.at[slot, :, pl.ds(0, wide)], w_sem.at[slot, 0]),
                pltpu.make_async_copy(wk.at[:, cols], w_s.at[slot, :, pl.ds(wide, HEAD)], w_sem.at[slot, 1]),
                pltpu.make_async_copy(wv.at[:, cols], w_s.at[slot, :, pl.ds(wide + HEAD, HEAD)], w_sem.at[slot, 2])]

    for c in weights(0, 0):
        c.start()

    for p in range(len(OPS)):
        ops_s[p] = _pick(me, OPS[p])
    for p in range(len(ITEMS)):
        items_s[p] = _pick(me, ITEMS[p])
    for p in range(len(ENDS)):
        ends_s[p] = _pick(me, ENDS[p])

    rows = 16
    gain = gain_ref[...].astype(jnp.float32)

    def norm(r, _):
        at = pl.ds(pl.multiple_of(r * rows, rows), rows)
        v = x_ref[at, :].astype(jnp.float32)
        scale = lax.rsqrt(jnp.mean(v * v, -1, keepdims=True) + 1e-6)
        a_s[at, :] = (v * scale * gain).astype(low)
        return _

    lax.fori_loop(0, t // rows, norm, 0)
    pl.semaphore_wait(barrier, RING - 1)

    def kv_copy(h, j, dest, arm):
        at = h * RING + j
        return pltpu.make_async_remote_copy(src_ref=kv_buf.at[h, j], dst_ref=kv_buf.at[h, j], send_sem=kv_sd.at[at * 2 + arm], recv_sem=kv_r.at[at],
                                            device_id={"sp": dest}, device_id_type=pl.DeviceIdType.MESH)

    def q_copy(h, i, dest):
        return pltpu.make_async_remote_copy(src_ref=q_buf.at[h, i], dst_ref=q_buf.at[h, i], send_sem=q_sd.at[h], recv_sem=q_r.at[h * RING + i],
                                            device_id={"sp": dest}, device_id_type=pl.DeviceIdType.MESH)

    def o_copy(h, slot, dest):
        cols = pl.ds(pl.multiple_of(h * wide, wide), wide)
        return pltpu.make_async_remote_copy(src_ref=o_st.at[slot], dst_ref=o_full.at[:, cols], send_sem=o_sd.at[slot], recv_sem=o_r.at[h],
                                            device_id={"sp": dest}, device_id_type=pl.DeviceIdType.MESH)

    def o_local(h, slot):
        cols = pl.ds(pl.multiple_of(h * wide, wide), wide)
        return pltpu.make_async_copy(o_st.at[slot], o_full.at[:, cols], ov_sem.at[0])

    def fields(word):
        return word & 7, (word >> 3) & 7, (word >> 6) & 15, (word >> 10) & 1, (word >> 11) & 1, (word >> 12) & 1

    def send(p, _):
        dest, j, h, waits, arm, queries = fields(ops_s[p])

        @pl.when(queries == 1)
        def _():
            q_copy(h, j, dest).start()

        @pl.when(queries == 0)
        def _():
            @pl.when(waits == 1)
            def _():
                kv_copy(h, j, other, 0).wait_recv()

            kv_copy(h, j, dest, arm).start()

        return 0

    def sends(s):
        lax.fori_loop(0 if isinstance(s, int) and s == 0 else ends_s[s - 1], ends_s[s], send, 0)

    def staged(h, slot):
        return [pltpu.make_async_copy(st_q.at[slot], q_buf.at[h, me], st_sem.at[slot, 0]),
                pltpu.make_async_copy(st_kv.at[slot], kv_buf.at[h, me], st_sem.at[slot, 1])]

    half = t // 2

    def project(h, r, slot):
        at = pl.ds(r * half, half)
        got = _dot(a_s[at, :], w_s[slot], 1, 0).astype(low)
        cos, sin = cos_ref[at, :], sin_ref[at, :]

        def turned(v):
            v = v.astype(jnp.float32)
            return (v * cos + pltpu.roll(v, HEAD // 2, 1) * sin).astype(low)

        for n in range(g):
            st_q[slot, pl.ds(n * t + r * half, half), :] = turned(got[:, n * HEAD : (n + 1) * HEAD])
        st_kv[slot, at, :] = turned(got[:, wide : wide + HEAD])
        for b in range(half // HEAD):
            st_kv[slot, pl.ds(t + r * half + b * HEAD, HEAD), :] = got[b * HEAD : (b + 1) * HEAD, wide + HEAD :].T

    def head(h, _):
        slot = lax.rem(h, 2)
        for c in weights(h, slot):
            c.wait()

        @pl.when(h + 1 < heads)
        def _():
            for c in weights(h + 1, 1 - slot):
                c.start()

        project(h, 0, slot)

        @pl.when(h >= 1)
        def _():
            for c in staged(h - 1, 1 - slot):
                c.wait()
            sends(h)

        project(h, 1, slot)
        for c in staged(h, slot):
            c.start()
        return 0

    lax.fori_loop(0, heads, head, 0)
    for c in staged(heads - 1, (heads - 1) % 2):
        c.wait()

    e = HEAD**-0.5 * LOG2E
    ones = jnp.ones((8, t), low)

    def block(j, masked):
        scores = [_dot(kvb[j, :t, :], q_v[n * t : (n + 1) * t, :], 1, 1) for n in range(g)]
        values = jnp.concatenate([jnp.concatenate([kvb[j, t + b * HEAD : t + (b + 1) * HEAD, :] for b in range(t // HEAD)], axis=1), ones], axis=0)
        kept = []
        for n, s in enumerate(scores):
            at = slice(n * t, (n + 1) * t)
            if masked:
                s = jnp.where(lax.broadcasted_iota(jnp.int32, s.shape, 0) <= lax.broadcasted_iota(jnp.int32, s.shape, 1), s, HIDDEN)
            old = top_s[:, at]
            top = jnp.maximum(old, s.max(axis=0, keepdims=True))
            top_s[:, at] = top
            kept.append((jnp.exp2((s - top) * e).astype(low), jnp.exp2((old - top) * e)))
        for n, (p, keep) in enumerate(kept):
            at = slice(n * t, (n + 1) * t)
            mix_s[:, at] = mix_s[:, at] * keep + _dot(values, p, 1, 0)

    def item(k, _):
        word = items_s[k]
        sends(heads + k)

        @pl.when(word >= 0)
        def _():
            i, h, q_wait, mask = word & 7, (word >> 3) & 15, (word >> 7) & 1, (word >> 8) & 255
            slot = lax.rem(k, 2)
            cp_q = pltpu.make_async_copy(q_buf.at[h, i], q_v, ld_sem.at[RING])

            def cp_kv(j):
                return pltpu.make_async_copy(kv_buf.at[h, j], kvb.at[j], ld_sem.at[j])

            @pl.when(q_wait == 1)
            def _():
                q_copy(h, i, other).wait_recv()

            cp_q.start()

            def arrive(j, _):
                @pl.when(((mask >> j) & 1) == 1)
                def _():
                    kv_copy(h, j, other, 0).wait_recv()

                cp_kv(j).start()
                return 0

            lax.fori_loop(0, i + 1, arrive, 0)
            top_s[...] = jnp.full(top_s.shape, NEG, jnp.float32)
            mix_s[...] = jnp.zeros(mix_s.shape, jnp.float32)
            cp_q.wait()

            def step(j, _):
                cp_kv(j).wait()
                block(j, False)
                return 0

            lax.fori_loop(0, i, step, 0)
            cp_kv(i).wait()
            block(i, True)

            @pl.when((k >= 2) & ((items_s[jnp.maximum(k - 2, 0)] & 7) != me))
            def _():
                o_copy(h, slot, other).wait_send()

            for n in range(g):
                at = slice(n * t, (n + 1) * t)
                o_st[slot, :, n * HEAD : (n + 1) * HEAD] = (mix_s[:HEAD, at] * (1 / mix_s[HEAD : HEAD + 1, at])).T.astype(low)

            @pl.when(i == me)
            def _():
                o_local(h, slot).start()
                o_local(h, slot).wait()

            @pl.when(i != me)
            def _():
                o_copy(h, slot, i).start()

        return 0

    part, width, rows = heads // 2 * wide, wo_s.shape[2], t // 2
    tiles = depth // width

    def project_out(half, last):
        def back(h, _):
            @pl.when(((_pick(me, AWAY) >> h) & 1) == 1)
            def _():
                o_copy(h, 0, other).wait_recv()

            return 0

        def tile(n, slot):
            return pltpu.make_async_copy(wo.at[pl.ds(half * part, part), pl.ds(pl.multiple_of(n * width, width), width)], wo_s.at[slot], wo_sem.at[slot])

        def out(n, slot):
            return pltpu.make_async_copy(y_st.at[slot], y_ref.at[:, pl.ds(pl.multiple_of(n * width, width), width)], y_sem.at[slot])

        tile(0, 0).start()
        lax.fori_loop(half * (heads // 2), (half + 1) * (heads // 2), back, 0)
        own = pltpu.make_async_copy(o_full.at[:, pl.ds(half * part, part)], o_v, ov_sem.at[0])
        own.start()
        own.wait()

        def column(n, _):
            slot = lax.rem(n, 2)
            cols = pl.ds(pl.multiple_of(n * width, width), width)
            tile(n, slot).wait()

            @pl.when(n + 1 < tiles)
            def _():
                tile(n + 1, 1 - slot).start()

            if last:

                @pl.when(n >= 2)
                def _():
                    out(n, slot).wait()

            def some(r, _):
                at = pl.ds(pl.multiple_of(r * rows, rows), rows)
                got = _dot(o_v[at, :], wo_s[slot], 1, 0)
                if last:
                    y_st[slot, at, :] = (x_ref[at, cols].astype(jnp.float32) + (y_s[at, cols] + got)).astype(low)
                else:
                    y_s[at, cols] = got
                return 0

            lax.fori_loop(0, t // rows, some, 0)
            if last:
                out(n, slot).start()
            return 0

        lax.fori_loop(0, tiles, column, 0)
        if last:
            for n in (tiles - 2, tiles - 1):
                out(n, n % 2).wait()

    early = _pick(me, EARLY)

    def step_of(k, _):
        @pl.when(k == early)
        def _():
            project_out(0, False)

        @pl.when(k < len(ITEMS))
        def _():
            item(k, 0)

        return 0

    lax.fori_loop(0, len(ITEMS) + 1, step_of, 0)
    sends(len(ENDS) - 1)
    project_out(1, True)

    def stored(k, _):
        after = items_s[jnp.minimum(k + 2, len(ITEMS) - 1)]

        @pl.when((items_s[k] >= 0) & ((items_s[k] & 7) != me) & ((k + 2 >= len(ITEMS)) | (after < 0)))
        def _():
            o_copy(0, lax.rem(k, 2), other).wait_send()

        return 0

    lax.fori_loop(0, len(ITEMS), stored, 0)

    def sent(p, _):
        dest, j, h, waits, arm, queries = fields(ops_s[p])

        @pl.when(queries == 1)
        def _():
            q_copy(h, j, dest).wait_send()

        @pl.when(queries == 0)
        def _():
            kv_copy(h, j, dest, arm).wait_send()

        return 0

    lax.fori_loop(0, ends_s[len(ENDS) - 1], sent, 0)


def attended(x, gain, wq, wk, wv, wo, cos, sin):
    t, depth = x.shape
    heads, g = wk.shape[1] // HEAD, wq.shape[1] // wk.shape[1]
    low = x.dtype
    width = 3 * HEAD if depth % (3 * HEAD) == 0 else HEAD
    anywhere, vmem = pl.BlockSpec(memory_space=pl.ANY), pl.BlockSpec(memory_space=pltpu.VMEM)
    dma = pltpu.SemaphoreType.DMA
    out = pl.pallas_call(
        functools.partial(_kernel, heads, g),
        out_shape=[jax.ShapeDtypeStruct((t, depth), low), jax.ShapeDtypeStruct((t, wq.shape[1]), low),
                   jax.ShapeDtypeStruct((heads, RING, 2 * t, HEAD), low),
                   jax.ShapeDtypeStruct((heads, RING, g * t, HEAD), low)],
        in_specs=[vmem] * 4 + [anywhere] * 4,
        out_specs=[anywhere] * 4,
        scratch_shapes=[
            pltpu.VMEM((t, depth), low),
            pltpu.VMEM((2, depth, (g + 2) * HEAD), low),
            pltpu.VMEM((2, g * t, HEAD), low),
            pltpu.VMEM((2, 2 * t, HEAD), low),
            pltpu.VMEM((RING, 2 * t, HEAD), low),
            pltpu.VMEM((g * t, HEAD), low),
            pltpu.VMEM((1, g * t), jnp.float32),
            pltpu.VMEM((HEAD + 8, g * t), jnp.float32),
            pltpu.VMEM((2, t, g * HEAD), low),
            pltpu.SMEM((len(OPS),), jnp.int32),
            pltpu.SMEM((len(ITEMS),), jnp.int32),
            pltpu.SMEM((len(ENDS),), jnp.int32),
            dma((heads * RING,)), dma((heads * RING,)), dma((heads,)), dma((heads * RING * 2,)), dma((heads,)), dma((2,)),
            dma((2, 3)), dma((2, 2)), dma((RING + 1,)),
            pltpu.VMEM((t, depth), jnp.float32),
            pltpu.VMEM((2, heads // 2 * g * HEAD, width), low),
            pltpu.VMEM((t, heads // 2 * g * HEAD), low),
            pltpu.VMEM((2, t, width), low),
            dma((2,)), dma((1,)), dma((2,)),
        ],
        compiler_params=pltpu.CompilerParams(collective_id=0, has_side_effects=True, vmem_limit_bytes=60 * 2**20),
    )(x, gain[None], cos, sin, wq, wk, wv, wo)
    return out[0]


def solution(mesh):
    def step(x, gain, wq, wk, wv, wo):
        own = x.shape[0]
        place = lax.axis_index("sp") * own + jnp.arange(own)
        half = HEAD // 2
        angle = place.astype(jnp.float32)[:, None] * THETA ** (-jnp.arange(half, dtype=jnp.float32) / half)
        cos, sin = jnp.cos(angle), jnp.sin(angle)
        return attended(x, gain, wq, wk, wv, wo, jnp.concatenate([cos, cos], 1), jnp.concatenate([-sin, sin], 1))

    tokens, whole = P(("dp", "sp"), None), P(None, None)
    return jax.shard_map(
        step,
        mesh=mesh,
        in_specs=(tokens, P(None), whole, whole, whole, whole),
        out_specs=tokens,
        check_vma=False,
    )
```

```python
import functools

import jax
import jax.numpy as jnp
from jax import lax
from jax.experimental import pallas as pl
from jax.experimental.pallas import tpu as pltpu
from jax.sharding import PartitionSpec as P

HEAD = 128
THETA = 10000
NEG = -1e30
HIDDEN = 2 * NEG
LOG2E = 1.4426950408889634
RING = 8
PLANS = [
    0o0023330064302326,
    0o0124466622555600,
    0o0122777733136415,
    0o0113555517426731,
    0o0224444476235650,
    0o0024444465370420,
    0o0111777761434253,
    0o0122277745111322,
    0o0223333277204326,
    0o0113331142621065,
    0o0122200073000435,
    0o0122220035343132,
    0o1133466611737754,
    0o0122556642745164,
    0o0113555517326715,
    0o0113331132351134,
]
START, PROJECT, BLOCK, PIECE, WIRE, FLIGHT = 8.0, 4.0, 0.95, 2.0, 5.6255, 2.0


def _way(a, b):
    d = (b - a) % RING
    return [(0, (a + k) % RING) for k in range(d)] if 2 * d < RING else [(1, (a - k) % RING) for k in range(RING - d)]


def _schedule():
    heads = len(PLANS)
    digits = [[(word >> 3 * (2 * RING - 1 - n)) & 7 for n in range(2 * RING)] for word in PLANS]
    place = [d[:RING] for d in digits]
    own = [[[] for _ in PLANS] for _ in range(RING)]
    relay, todo, need = {}, [[] for _ in range(RING)], {}
    for h, d in enumerate(digits):
        for j in range(RING):
            users = {place[h][i] for i in range(j, RING)}
            for arm in range(2):
                hops = [o for o in range(1, RING) if (o <= d[RING + j] if arm == 0 else RING - o > d[RING + j])]
                chain = [n for n in ((j + o) % RING if arm == 0 else (j - o) % RING for o in hops) if n in users]
                for k, (a, b) in enumerate(zip([j] + chain, chain)):
                    move = ("kv", h, j, a, b, arm)
                    if a == j:
                        own[j][h].append((k - len(chain) - 0.01 * len(_way(a, b)), move))
                    else:
                        relay[h, j, a] = move
            if place[h][j] != j:
                own[j][h].append((-1.5 - 0.01 * len(_way(j, place[h][j])), ("q", h, j, j, place[h][j], 0)))
            m = place[h][j]
            todo[m].append((h, j))
            need[h, j] = {("kv", h, n) for n in range(j + 1) if n != m} | ({("q", h, j)} if j != m else set())
    count = [len(t) for t in todo]
    ops, items, ends = [[] for _ in range(RING)], [[] for _ in range(RING)], [[0] for _ in range(RING)]
    heard = [set() for _ in range(RING)]
    queue = {(m, way): [] for m in range(RING) for way in range(2)}
    live, late, flying = {}, [[] for _ in range(RING)], []
    step, at, idle, busy = [1] * RING, [START + 1.5 * PROJECT] * RING, [False] * RING, [None] * RING
    now = 0.0

    def push(move):
        kind, h, j, a, b, arm = move
        queue[a, _way(a, b)[0][0]].append(move)
        if kind != "o":
            waits = kind == "kv" and a != j
            if waits:
                heard[a].add((h, j))
            ops[a].append(b | j << 3 | h << 6 | waits << 10 | arm << 11 | (kind == "q") << 12)

    def begin(m):
        for h, i in todo[m]:
            if not need[h, i]:
                todo[m].remove((h, i))
                mask = sum(1 << n for n in range(i + 1) if n != m and (h, n) not in heard[m])
                heard[m].update((h, n) for n in range(i + 1))
                items[m].append(i | h << 3 | (i != m) << 7 | mask << 8)
                ends[m].append(len(ops[m]))
                busy[m], idle[m], at[m] = (h, i), False, now + PIECE + BLOCK * (i + 1)
                return
        idle[m], at[m] = True, float("inf")

    while True:
        for key, waiting in queue.items():
            if waiting and key not in live:
                live[key] = [waiting.pop(0), 1.0]
        room, users = {}, {}
        for key, (move, _) in live.items():
            for link in _way(move[3], move[4]):
                room[link] = 1 / WIRE
                users.setdefault(link, set()).add(key)
        rate = {}
        while len(rate) < len(live):
            link = min((n for n in users if users[n]), key=lambda n: room[n] / len(users[n]))
            share = room[link] / len(users[link])
            for key in sorted(users[link]):
                rate[key] = share
                for n in _way(live[key][0][3], live[key][0][4]):
                    room[n] -= share
                    users[n].discard(key)
        then = min([now + left / rate[key] for key, (_, left) in live.items()] + at + [t for t, _ in flying[:1]])
        if then == float("inf"):
            break
        for key in list(live):
            live[key][1] -= rate[key] * (then - now)
            if live[key][1] < 1e-8:
                flying.append((then + FLIGHT, live.pop(key)[0]))
        now = then
        while flying and flying[0][0] <= now + 1e-9:
            kind, h, j, _, m, _ = flying.pop(0)[1]
            if kind == "o":
                continue
            if kind == "kv" and (h, j, m) in relay:
                (push if idle[m] else late[m].append)(relay[h, j, m])
            for i in range(RING):
                if place[h][i] == m:
                    need[h, i].discard((kind, h, j))
            if idle[m]:
                begin(m)
        for m in range(RING):
            while at[m] <= now + 1e-9:
                s = step[m]
                step[m] += 1
                if s <= heads:
                    for _, move in sorted(own[m][s - 1]):
                        push(move)
                elif busy[m] and busy[m][1] != m:
                    push(("o", *busy[m], m, busy[m][1], 0))
                for move in late[m]:
                    push(move)
                late[m] = []
                if s < heads:
                    ends[m].append(len(ops[m]))
                    at[m] = START + (s + 1.5) * PROJECT if s + 1 < heads else START + heads * PROJECT + 0.5
                else:
                    begin(m)
    last = max(count)
    for m in range(RING):
        items[m] += [-1] * (last - len(items[m]))
        ends[m] += [len(ops[m])] * (heads + last + 1 - len(ends[m]))
    longest = max(len(o) for o in ops)
    ops = [o + [0] * (longest - len(o)) for o in ops]
    away = [sum(1 << h for h in range(heads) if place[h][m] != m) for m in range(RING)]
    return *([list(row) for row in zip(*table)] for table in (ops, items, ends)), away, now


OPS, ITEMS, ENDS, AWAY, _ = _schedule()


def _dot(a, b, ca, cb):
    return lax.dot_general(a, b, (((ca,), (cb,)), ((), ())), preferred_element_type=jnp.float32)


def _pick(me, values):
    got = jnp.int32(values[0])
    for d in range(1, len(values)):
        got = jnp.where(me == d, jnp.int32(values[d]), got)
    return got


def _kernel(heads, g, x_ref, gain_ref, cos_ref, sin_ref, wq, wk, wv, o_full, kv_buf, q_buf, a_s, w_s, st_q, st_kv, kvb, q_v, top_s, mix_s, o_st,
            ops_s, items_s, ends_s, kv_r, q_r, o_r, kv_sd, q_sd, o_sd, w_sem, st_sem, ld_sem):
    me = lax.axis_index("sp")
    t, depth = x_ref.shape
    wide = g * HEAD
    low = x_ref.dtype
    other = lax.rem(me + 1, RING)

    barrier = pltpu.get_barrier_semaphore()
    for k in range(1, RING):
        pl.semaphore_signal(barrier, inc=1, device_id={"sp": lax.rem(me + k, RING)}, device_id_type=pl.DeviceIdType.MESH)

    def weights(h, slot):
        q_cols = pl.ds(pl.multiple_of(h * wide, wide), wide)
        cols = pl.ds(pl.multiple_of(h * HEAD, HEAD), HEAD)
        return [pltpu.make_async_copy(wq.at[:, q_cols], w_s.at[slot, :, pl.ds(0, wide)], w_sem.at[slot, 0]),
                pltpu.make_async_copy(wk.at[:, cols], w_s.at[slot, :, pl.ds(wide, HEAD)], w_sem.at[slot, 1]),
                pltpu.make_async_copy(wv.at[:, cols], w_s.at[slot, :, pl.ds(wide + HEAD, HEAD)], w_sem.at[slot, 2])]

    for c in weights(0, 0):
        c.start()

    for p in range(len(OPS)):
        ops_s[p] = _pick(me, OPS[p])
    for p in range(len(ITEMS)):
        items_s[p] = _pick(me, ITEMS[p])
    for p in range(len(ENDS)):
        ends_s[p] = _pick(me, ENDS[p])

    rows = 16
    gain = gain_ref[...].astype(jnp.float32)

    def norm(r, _):
        at = pl.ds(pl.multiple_of(r * rows, rows), rows)
        v = x_ref[at, :].astype(jnp.float32)
        scale = lax.rsqrt(jnp.mean(v * v, -1, keepdims=True) + 1e-6)
        a_s[at, :] = (v * scale * gain).astype(low)
        return _

    lax.fori_loop(0, t // rows, norm, 0)
    pl.semaphore_wait(barrier, RING - 1)

    def kv_copy(h, j, dest, arm):
        at = h * RING + j
        return pltpu.make_async_remote_copy(src_ref=kv_buf.at[h, j], dst_ref=kv_buf.at[h, j], send_sem=kv_sd.at[at * 2 + arm], recv_sem=kv_r.at[at],
                                            device_id={"sp": dest}, device_id_type=pl.DeviceIdType.MESH)

    def q_copy(h, i, dest):
        return pltpu.make_async_remote_copy(src_ref=q_buf.at[h, i], dst_ref=q_buf.at[h, i], send_sem=q_sd.at[h], recv_sem=q_r.at[h * RING + i],
                                            device_id={"sp": dest}, device_id_type=pl.DeviceIdType.MESH)

    def o_copy(h, slot, dest):
        cols = pl.ds(pl.multiple_of(h * wide, wide), wide)
        return pltpu.make_async_remote_copy(src_ref=o_st.at[slot], dst_ref=o_full.at[:, cols], send_sem=o_sd.at[slot], recv_sem=o_r.at[h],
                                            device_id={"sp": dest}, device_id_type=pl.DeviceIdType.MESH)

    def o_local(h, slot):
        cols = pl.ds(pl.multiple_of(h * wide, wide), wide)
        return pltpu.make_async_copy(o_st.at[slot], o_full.at[:, cols], o_sd.at[slot])

    def fields(word):
        return word & 7, (word >> 3) & 7, (word >> 6) & 15, (word >> 10) & 1, (word >> 11) & 1, (word >> 12) & 1

    def send(p, _):
        dest, j, h, waits, arm, queries = fields(ops_s[p])

        @pl.when(queries == 1)
        def _():
            q_copy(h, j, dest).start()

        @pl.when(queries == 0)
        def _():
            @pl.when(waits == 1)
            def _():
                kv_copy(h, j, other, 0).wait_recv()

            kv_copy(h, j, dest, arm).start()

        return 0

    def sends(s):
        lax.fori_loop(0 if isinstance(s, int) and s == 0 else ends_s[s - 1], ends_s[s], send, 0)

    def staged(h, slot):
        return [pltpu.make_async_copy(st_q.at[slot], q_buf.at[h, me], st_sem.at[slot, 0]),
                pltpu.make_async_copy(st_kv.at[slot], kv_buf.at[h, me], st_sem.at[slot, 1])]

    half = t // 2

    def project(h, r, slot):
        at = pl.ds(r * half, half)
        got = _dot(a_s[at, :], w_s[slot], 1, 0).astype(low)
        cos, sin = cos_ref[at, :], sin_ref[at, :]

        def turned(v):
            v = v.astype(jnp.float32)
            return (v * cos + pltpu.roll(v, HEAD // 2, 1) * sin).astype(low)

        for n in range(g):
            st_q[slot, pl.ds(n * t + r * half, half), :] = turned(got[:, n * HEAD : (n + 1) * HEAD])
        st_kv[slot, at, :] = turned(got[:, wide : wide + HEAD])
        for b in range(half // HEAD):
            st_kv[slot, pl.ds(t + r * half + b * HEAD, HEAD), :] = got[b * HEAD : (b + 1) * HEAD, wide + HEAD :].T

    def head(h, _):
        slot = lax.rem(h, 2)
        for c in weights(h, slot):
            c.wait()

        @pl.when(h + 1 < heads)
        def _():
            for c in weights(h + 1, 1 - slot):
                c.start()

        project(h, 0, slot)

        @pl.when(h >= 1)
        def _():
            for c in staged(h - 1, 1 - slot):
                c.wait()
            sends(h)

        project(h, 1, slot)
        for c in staged(h, slot):
            c.start()
        return 0

    lax.fori_loop(0, heads, head, 0)
    for c in staged(heads - 1, (heads - 1) % 2):
        c.wait()

    e = HEAD**-0.5 * LOG2E
    ones = jnp.ones((8, t), low)

    def block(j, masked):
        scores = [_dot(kvb[j, :t, :], q_v[n * t : (n + 1) * t, :], 1, 1) for n in range(g)]
        values = jnp.concatenate([jnp.concatenate([kvb[j, t + b * HEAD : t + (b + 1) * HEAD, :] for b in range(t // HEAD)], axis=1), ones], axis=0)
        kept = []
        for n, s in enumerate(scores):
            at = slice(n * t, (n + 1) * t)
            if masked:
                s = jnp.where(lax.broadcasted_iota(jnp.int32, s.shape, 0) <= lax.broadcasted_iota(jnp.int32, s.shape, 1), s, HIDDEN)
            old = top_s[:, at]
            top = jnp.maximum(old, s.max(axis=0, keepdims=True))
            top_s[:, at] = top
            kept.append((jnp.exp2((s - top) * e).astype(low), jnp.exp2((old - top) * e)))
        for n, (p, keep) in enumerate(kept):
            at = slice(n * t, (n + 1) * t)
            mix_s[:, at] = mix_s[:, at] * keep + _dot(values, p, 1, 0)

    def item(k, _):
        word = items_s[k]
        sends(heads + k)

        @pl.when(word >= 0)
        def _():
            i, h, q_wait, mask = word & 7, (word >> 3) & 15, (word >> 7) & 1, (word >> 8) & 255
            slot = lax.rem(k, 2)
            cp_q = pltpu.make_async_copy(q_buf.at[h, i], q_v, ld_sem.at[RING])

            def cp_kv(j):
                return pltpu.make_async_copy(kv_buf.at[h, j], kvb.at[j], ld_sem.at[j])

            @pl.when(q_wait == 1)
            def _():
                q_copy(h, i, other).wait_recv()

            cp_q.start()

            def arrive(j, _):
                @pl.when(((mask >> j) & 1) == 1)
                def _():
                    kv_copy(h, j, other, 0).wait_recv()

                cp_kv(j).start()
                return 0

            lax.fori_loop(0, i + 1, arrive, 0)
            top_s[...] = jnp.full(top_s.shape, NEG, jnp.float32)
            mix_s[...] = jnp.zeros(mix_s.shape, jnp.float32)
            cp_q.wait()

            def step(j, _):
                cp_kv(j).wait()
                block(j, False)
                return 0

            lax.fori_loop(0, i, step, 0)
            cp_kv(i).wait()
            block(i, True)

            @pl.when(k >= 2)
            def _():
                o_local(h, slot).wait()

            for n in range(g):
                at = slice(n * t, (n + 1) * t)
                o_st[slot, :, n * HEAD : (n + 1) * HEAD] = (mix_s[:HEAD, at] * (1 / mix_s[HEAD : HEAD + 1, at])).T.astype(low)

            @pl.when(i == me)
            def _():
                o_local(h, slot).start()

            @pl.when(i != me)
            def _():
                o_copy(h, slot, i).start()

        return 0

    lax.fori_loop(0, len(ITEMS), item, 0)
    sends(len(ENDS) - 1)

    for slot in range(2):
        o_local(0, slot).wait()

    def sent(p, _):
        dest, j, h, waits, arm, queries = fields(ops_s[p])

        @pl.when(queries == 1)
        def _():
            q_copy(h, j, dest).wait_send()

        @pl.when(queries == 0)
        def _():
            kv_copy(h, j, dest, arm).wait_send()

        return 0

    lax.fori_loop(0, ends_s[len(ENDS) - 1], sent, 0)

    def back(h, _):
        @pl.when(((_pick(me, AWAY) >> h) & 1) == 1)
        def _():
            o_copy(h, 0, other).wait_recv()

        return 0

    lax.fori_loop(0, heads, back, 0)


def attended(x, gain, wq, wk, wv, cos, sin):
    t, depth = x.shape
    heads, g = wk.shape[1] // HEAD, wq.shape[1] // wk.shape[1]
    low = x.dtype
    anywhere, vmem = pl.BlockSpec(memory_space=pl.ANY), pl.BlockSpec(memory_space=pltpu.VMEM)
    dma = pltpu.SemaphoreType.DMA
    out = pl.pallas_call(
        functools.partial(_kernel, heads, g),
        out_shape=[jax.ShapeDtypeStruct((t, wq.shape[1]), low), jax.ShapeDtypeStruct((heads, RING, 2 * t, HEAD), low),
                   jax.ShapeDtypeStruct((heads, RING, g * t, HEAD), low)],
        in_specs=[vmem] * 4 + [anywhere] * 3,
        out_specs=[anywhere] * 3,
        scratch_shapes=[
            pltpu.VMEM((t, depth), low),
            pltpu.VMEM((2, depth, (g + 2) * HEAD), low),
            pltpu.VMEM((2, g * t, HEAD), low),
            pltpu.VMEM((2, 2 * t, HEAD), low),
            pltpu.VMEM((RING, 2 * t, HEAD), low),
            pltpu.VMEM((g * t, HEAD), low),
            pltpu.VMEM((1, g * t), jnp.float32),
            pltpu.VMEM((HEAD + 8, g * t), jnp.float32),
            pltpu.VMEM((2, t, g * HEAD), low),
            pltpu.SMEM((len(OPS),), jnp.int32),
            pltpu.SMEM((len(ITEMS),), jnp.int32),
            pltpu.SMEM((len(ENDS),), jnp.int32),
            dma((heads * RING,)), dma((heads * RING,)), dma((heads,)), dma((heads * RING * 2,)), dma((heads,)), dma((2,)),
            dma((2, 3)), dma((2, 2)), dma((RING + 1,)),
        ],
        compiler_params=pltpu.CompilerParams(collective_id=0, has_side_effects=True, vmem_limit_bytes=60 * 2**20),
    )(x, gain[None], cos, sin, wq, wk, wv)
    return out[0]


def solution(mesh):
    def step(x, gain, wq, wk, wv, wo):
        own = x.shape[0]
        place = lax.axis_index("sp") * own + jnp.arange(own)
        half = HEAD // 2
        angle = place.astype(jnp.float32)[:, None] * THETA ** (-jnp.arange(half, dtype=jnp.float32) / half)
        cos, sin = jnp.cos(angle), jnp.sin(angle)
        seen = attended(x, gain, wq, wk, wv, jnp.concatenate([cos, cos], 1), jnp.concatenate([-sin, sin], 1))
        y = jnp.dot(seen, wo, preferred_element_type=jnp.float32)
        return (x.astype(jnp.float32) + y).astype(jnp.bfloat16)

    tokens, whole = P(("dp", "sp"), None), P(None, None)
    return jax.shard_map(
        step,
        mesh=mesh,
        in_specs=(tokens, P(None), whole, whole, whole, whole),
        out_specs=tokens,
        check_vma=False,
    )
```
